8 devices in a mesh: stage: 2 (over z, y), data: 4 (over x, core).
Axes of the slice: x: 2, y: 2, z: 1, core: 2. Of those that a mesh axis runs over, the one named last changes fastest.
Arguments:
- x_in: bfloat16 [32, 2048, 768], P(None, 'data')
- targets: bfloat16 [32, 2048, 768], P(None, 'data')
- w1_bf: bfloat16 [2, 2, 1, 768, 3072], P('stage')
- w2_bf: bfloat16 [2, 2, 1, 3072, 768], P('stage')
- w_master: float32 [2, 2, 1, 4718592], P('stage', None, None, 'data')
- m_state: float32 [2, 2, 1, 4718592], P('stage', None, None, 'data')
- v_state: float32 [2, 2, 1, 4718592], P('stage', None, None, 'data')
Outputs:
- output 1: bfloat16 [2, 2, 1, 768, 3072], P('stage')
- output 2: bfloat16 [2, 2, 1, 3072, 768], P('stage')
- output 3: float32 [2, 2, 1, 4718592], P('stage', None, None, 'data')
- output 4: float32 [2, 2, 1, 4718592], P('stage', None, None, 'data')
- output 5: float32 [2, 2, 1, 4718592], P('stage', None, None, 'data')
- output 6: float32 [], replicated
All inputs are finite; a program needn't handle non-finite values.
Results may differ from the reference program's by a relative error of at most 0.001.
Values are sent between devices in bfloat16 or wider.
A program may use at most 1 GiB of HBM per device.

```python
import math
import jax
import jax.numpy as jnp
from jax import lax

STAGES = 2
DATA_WAYS = 4
MB_GROUPS = 16
TOK_DEV = 512
VSTAGE_BLOCKS = 1
D_MODEL = 768
ADAM_STEP = 1000

N_MICRO = MB_GROUPS * STAGES
N_ROWS = DATA_WAYS * TOK_DEV
D_FF = 4 * D_MODEL
N_BLOCKS = 2 * STAGES * VSTAGE_BLOCKS
N_TOKENS = N_MICRO * N_ROWS
FLAT_LEN = 8 * D_MODEL * D_MODEL
N_PARAMS = N_BLOCKS * FLAT_LEN
BETA_ONE = 0.9
BETA_TWO = 0.999
ADAM_EPS = 1e-8
WEIGHT_DECAY = 0.1
TAU_CLIP = 0.3 * D_MODEL * math.sqrt(N_BLOCKS * (3.0 / N_TOKENS + 0.008))
LEARN_RATE = 0.1 / math.sqrt(4.0 * D_MODEL * N_BLOCKS)


def gelu_tanh(pre_act):
    return jax.nn.gelu(pre_act, approximate=True)


def moment_scale():
    scale_two = TAU_CLIP * math.sqrt(2.0 / (N_PARAMS * (1.0 + 1.0 / N_BLOCKS)))
    scale_one = scale_two / math.sqrt(N_BLOCKS)
    return jnp.concatenate([jnp.full((D_MODEL * D_FF,), scale_one, jnp.float32), jnp.full((D_FF * D_MODEL,), scale_two, jnp.float32)])


def setup_inputs(seed: int = 0) -> dict:
    key_list = jax.random.split(jax.random.key(seed), 6)
    act_shape = (N_MICRO, N_ROWS, D_MODEL)
    lead_dims = (STAGES, 2, VSTAGE_BLOCKS)
    x_in = jax.random.normal(key_list[0], act_shape, jnp.float32)
    targets = jax.random.normal(key_list[1], act_shape, jnp.float32)
    w_one = jax.random.normal(key_list[2], lead_dims + (D_MODEL, D_FF), jnp.float32) * D_MODEL ** -0.5
    w_two = jax.random.normal(key_list[3], lead_dims + (D_FF, D_MODEL), jnp.float32) * (D_FF * N_BLOCKS) ** -0.5
    w_master = jnp.concatenate([w_one.reshape(lead_dims + (-1,)), w_two.reshape(lead_dims + (-1,))], axis=-1)
    elem_scale = moment_scale()
    m_state = 0.5 * elem_scale * jax.random.normal(key_list[4], w_master.shape, jnp.float32)
    v_state = elem_scale * elem_scale * (0.25 + 0.5 * jax.random.uniform(key_list[5], w_master.shape, jnp.float32))
    return dict(x_in=x_in.astype(jnp.bfloat16), targets=targets.astype(jnp.bfloat16), w1_bf=w_one.astype(jnp.bfloat16), w2_bf=w_two.astype(jnp.bfloat16), w_master=w_master, m_state=m_state, v_state=v_state)


def block_forward(h_in, w_one, w_two):
    pre_act = jnp.dot(h_in, w_one, preferred_element_type=jnp.float32)
    act_bf = gelu_tanh(pre_act).astype(jnp.bfloat16)
    out_val = h_in.astype(jnp.float32) + jnp.dot(act_bf, w_two, preferred_element_type=jnp.float32)
    return out_val.astype(jnp.bfloat16)


def block_backward(h_in, grad_out, w_one, w_two):
    pre_act = jnp.dot(h_in, w_one, preferred_element_type=jnp.float32)
    act_val, gelu_pull = jax.vjp(gelu_tanh, pre_act)
    act_bf = act_val.astype(jnp.bfloat16)
    grad_act = jnp.dot(grad_out, w_two.T, preferred_element_type=jnp.float32)
    grad_pre = gelu_pull(grad_act)[0].astype(jnp.bfloat16)
    back_val = jnp.dot(grad_pre, w_one.T, preferred_element_type=jnp.float32)
    grad_in = (grad_out.astype(jnp.float32) + back_val).astype(jnp.bfloat16)
    grad_one = jnp.dot(h_in.T, grad_pre, preferred_element_type=jnp.float32)
    grad_two = jnp.dot(act_bf.T, grad_out, preferred_element_type=jnp.float32)
    return grad_in, grad_one, grad_two


def reference(x_in, targets, w1_bf, w2_bf, w_master, m_state, v_state):
    w_ones = jnp.swapaxes(w1_bf, 0, 1).reshape(N_BLOCKS, D_MODEL, D_FF)
    w_twos = jnp.swapaxes(w2_bf, 0, 1).reshape(N_BLOCKS, D_FF, D_MODEL)

    def fwd_step(h_in, weights):
        return block_forward(h_in, weights[0], weights[1]), h_in

    def bwd_step(grad_out, saved_item):
        grad_in, grad_one, grad_two = block_backward(saved_item[0], grad_out, saved_item[1], saved_item[2])
        return grad_in, (grad_one, grad_two)

    def micro_step(state_carry, mb_pair):
        acc_one, acc_two, loss_acc = state_carry
        h_out, block_inputs = lax.scan(fwd_step, mb_pair[0], (w_ones, w_twos))
        residual = h_out.astype(jnp.float32) - mb_pair[1].astype(jnp.float32)
        loss_acc = loss_acc + 0.5 * jnp.sum(residual * residual)
        grad_seed = (residual / N_TOKENS).astype(jnp.bfloat16)
        grad_pair = lax.scan(bwd_step, grad_seed, (block_inputs, w_ones, w_twos), reverse=True)[1]
        return (acc_one + grad_pair[0], acc_two + grad_pair[1], loss_acc), None

    start_carry = (jnp.zeros((N_BLOCKS, D_MODEL, D_FF), jnp.float32), jnp.zeros((N_BLOCKS, D_FF, D_MODEL), jnp.float32), jnp.zeros((), jnp.float32))
    acc_one, acc_two, loss_acc = lax.scan(micro_step, start_carry, (x_in, targets))[0]
    flat_dims = (2, STAGES, VSTAGE_BLOCKS, -1)
    grad_flat = jnp.swapaxes(jnp.concatenate([acc_one.reshape(flat_dims), acc_two.reshape(flat_dims)], axis=-1), 0, 1)
    grad_norm = jnp.sqrt(jnp.sum(grad_flat * grad_flat))
    clip_factor = jnp.minimum(1.0, TAU_CLIP / grad_norm)
    grad_clip = clip_factor * grad_flat
    m_new = BETA_ONE * m_state + (1.0 - BETA_ONE) * grad_clip
    v_new = BETA_TWO * v_state + (1.0 - BETA_TWO) * grad_clip * grad_clip
    m_hat = m_new / (1.0 - BETA_ONE ** ADAM_STEP)
    v_hat = v_new / (1.0 - BETA_TWO ** ADAM_STEP)
    w_new = w_master - LEARN_RATE * (m_hat / (jnp.sqrt(v_hat) + ADAM_EPS) + WEIGHT_DECAY * w_master)
    w_bf = w_new.astype(jnp.bfloat16)
    split_at = D_MODEL * D_FF
    w1_new = w_bf[..., :split_at].reshape(STAGES, 2, VSTAGE_BLOCKS, D_MODEL, D_FF)
    w2_new = w_bf[..., split_at:].reshape(STAGES, 2, VSTAGE_BLOCKS, D_FF, D_MODEL)
    return w1_new, w2_new, w_new, m_new, v_new, loss_acc / N_TOKENS
```

```python
import math
import jax
import jax.numpy as jnp
from jax import lax
from jax.experimental import pallas as pl
from jax.experimental.pallas import tpu as pltpu
from jax.sharding import PartitionSpec as P

BETA_ONE = 0.9
BETA_TWO = 0.999
ADAM_EPS = 1e-8
WEIGHT_DECAY = 0.1
ADAM_STEP = 1000
BF = jnp.bfloat16
F32 = jnp.float32
K_GELU = math.sqrt(2.0 / math.pi)
C_GELU = 0.044715
ANY = pl.ANY
TM = 512
N_PART = 3
VMEM_CAP = 60 * 1024 * 1024


def dot_nn(lhs, rhs):
    return lax.dot_general(lhs, rhs, (((1,), (0,)), ((), ())), preferred_element_type=F32)


def dot_nt(lhs, rhs):
    return lax.dot_general(lhs, rhs, (((1,), (1,)), ((), ())), preferred_element_type=F32)


def dot_tn(lhs, rhs):
    return lax.dot_general(lhs, rhs, (((0,), (0,)), ((), ())), preferred_element_type=F32)


def gelu_and_slope(u):
    sq = u * u
    half = 0.5 + 0.5 * jnp.tanh(u * (K_GELU + (K_GELU * C_GELU) * sq))
    act = u * half
    slope = half + (act * (1.0 - half)) * (2.0 * K_GELU + (6.0 * K_GELU * C_GELU) * sq)
    return act, slope


def row_spec(width, moved=False):
    if moved:
        return pl.BlockSpec((TM, width), lambda i, off: (i + off[0], 0))
    return pl.BlockSpec((TM, width), lambda i, off: (i, 0))


def weight_spec(r, c, which):
    return pl.BlockSpec((None, r, c), lambda i, off: (which, 0, 0), pipeline_mode=pl.Buffered(1))


def fwd_call(first, x, w_one, w_two, which, n_row, targets=None, n_tokens=None, chunk=1024):
    d_model = x.shape[1]
    d_ff = w_one.shape[2]
    last = targets is not None

    def kernel(off_ref, x_ref, w1_ref, w2_ref, *rest):
        if last:
            t_ref, h_ref, a_ref, s_ref, loss_ref = rest
        else:
            h_ref, a_ref, s_ref = rest
        acc = x_ref[...].astype(F32)
        pre = dot_nn(x_ref[...], w1_ref[:, :chunk])
        for lo in range(0, d_ff, chunk):
            cols = slice(lo, lo + chunk)
            ahead = dot_nn(x_ref[...], w1_ref[:, lo + chunk:lo + 2 * chunk]) if lo + chunk < d_ff else None
            act, slope = gelu_and_slope(pre)
            act = act.astype(BF)
            a_ref[:, cols] = act
            s_ref[:, cols] = slope
            acc = acc + dot_nn(act, w2_ref[cols, :])
            pre = ahead
        out = acc.astype(BF)
        if not last:
            h_ref[...] = out
        else:
            residual = out.astype(F32) - t_ref[...].astype(F32)
            h_ref[...] = (residual / n_tokens).astype(BF)
            part = jnp.sum((residual * residual).reshape(TM // 8, 8, d_model), axis=0)

            @pl.when(pl.program_id(0) == 0)
            def _():
                loss_ref[...] = part

            @pl.when(pl.program_id(0) > 0)
            def _():
                loss_ref[...] += part

    out_specs = [row_spec(d_model), row_spec(d_ff), row_spec(d_ff)]
    out_shape = [jax.ShapeDtypeStruct((n_row, d_model), BF), jax.ShapeDtypeStruct((n_row, d_ff), BF), jax.ShapeDtypeStruct((n_row, d_ff), F32)]
    if last:
        out_specs.append(pl.BlockSpec((8, d_model), lambda i, off: (0, 0)))
        out_shape.append(jax.ShapeDtypeStruct((8, d_model), F32))
    return pl.pallas_call(
        kernel,
        grid_spec=pltpu.PrefetchScalarGridSpec(
            num_scalar_prefetch=1, grid=(n_row // TM,),
            in_specs=[row_spec(d_model), weight_spec(d_model, d_ff, which), weight_spec(d_ff, d_model, which)] + ([row_spec(d_model, True)] if last else []),
            out_specs=out_specs),
        out_shape=out_shape,
        compiler_params=pltpu.CompilerParams(vmem_limit_bytes=VMEM_CAP, dimension_semantics=("arbitrary",)),
        cost_estimate=pl.CostEstimate(flops=4 * n_row * d_model * d_ff, bytes_accessed=n_row * d_ff * 6, transcendentals=n_row * d_ff),
        name="block_fwd",
    )(first, x, w_one, w_two, *([targets] if last else []))


def up_call(first, x, w_one, which, n_row, chunk=1024):
    d_model = x.shape[1]
    d_ff = w_one.shape[2]

    def kernel(off_ref, x_ref, w1_ref, a_ref, s_ref):
        for lo in range(0, d_ff, chunk):
            cols = slice(lo, lo + chunk)
            act, slope = gelu_and_slope(dot_nn(x_ref[...], w1_ref[:, cols]))
            a_ref[:, cols] = act.astype(BF)
            s_ref[:, cols] = slope

    return pl.pallas_call(
        kernel,
        grid_spec=pltpu.PrefetchScalarGridSpec(
            num_scalar_prefetch=1, grid=(n_row // TM,),
            in_specs=[row_spec(d_model, True), weight_spec(d_model, d_ff, which)],
            out_specs=[row_spec(d_ff), row_spec(d_ff)]),
        out_shape=[jax.ShapeDtypeStruct((n_row, d_ff), BF), jax.ShapeDtypeStruct((n_row, d_ff), F32)],
        compiler_params=pltpu.CompilerParams(vmem_limit_bytes=VMEM_CAP, dimension_semantics=("arbitrary",)),
        cost_estimate=pl.CostEstimate(flops=2 * n_row * d_model * d_ff, bytes_accessed=n_row * d_ff * 6, transcendentals=n_row * d_ff),
        name="block_up",
    )(first, x, w_one)


def down_call(first, x, act, w_two, which, n_row):
    d_model = x.shape[1]
    d_ff = w_two.shape[1]

    def kernel(off_ref, x_ref, a_ref, w2_ref, h_ref):
        h_ref[...] = (x_ref[...].astype(F32) + dot_nn(a_ref[...], w2_ref[...])).astype(BF)

    return pl.pallas_call(
        kernel,
        grid_spec=pltpu.PrefetchScalarGridSpec(
            num_scalar_prefetch=1, grid=(n_row // TM,),
            in_specs=[row_spec(d_model, True), row_spec(d_ff), weight_spec(d_ff, d_model, which)],
            out_specs=row_spec(d_model)),
        out_shape=jax.ShapeDtypeStruct((n_row, d_model), BF),
        compiler_params=pltpu.CompilerParams(vmem_limit_bytes=VMEM_CAP, dimension_semantics=("arbitrary",)),
        cost_estimate=pl.CostEstimate(flops=2 * n_row * d_model * d_ff, bytes_accessed=n_row * d_ff * 2, transcendentals=0),
        name="block_down",
    )(first, x, act, w_two)


def bwd_call(first, x, grad, act, slope, w_one, w_two, which, pair, n_part=1, chunk=1024):
    n_row, d_model = grad.shape
    d_ff = w_one.shape[2]
    n_step = n_row // TM
    lanes = d_ff // 128
    major = d_model // 8
    per = d_ff // d_model
    part_lanes = lanes // n_part
    pair_shape = (2, 2, major, part_lanes, 8, 128)

    def kernel(off_ref, x_ref, g_ref, a_ref, s_ref, w1_ref, w2_ref, *rest):
        if pair is not None:
            rest = rest[n_part:]
        gin_ref, pair_refs, (acc1, acc2, sem) = rest[0], rest[1:1 + n_part], rest[1 + n_part:]
        step = pl.program_id(0)

        @pl.when(step == 0)
        def _():
            acc1[...] = jnp.zeros_like(acc1)
            acc2[...] = jnp.zeros_like(acc2)

        back = g_ref[...].astype(F32)
        for lo in range(0, d_ff, chunk):
            cols = slice(lo, lo + chunk)
            r = (dot_nt(g_ref[...], w2_ref[cols, :]) * s_ref[:, cols]).astype(BF)
            acc1[:, :, cols] += dot_tn(x_ref[...], r).reshape(major, 8, chunk)
            n_grp = chunk // (8 * per)
            acc2[lo // (8 * per):lo // (8 * per) + n_grp] += dot_tn(a_ref[:, cols], g_ref[...]).reshape(n_grp, per, 8, d_model)
            back = back + dot_nt(r, w1_ref[:, cols])
        gin_ref[...] = back.astype(BF)

        @pl.when(step == n_step - 1)
        def _():
            copies = []
            for lane in range(lanes):
                part, slot = lane // part_lanes, lane % part_lanes
                wide = part_lanes // per
                col = part * wide + slot % wide
                copies.append(pltpu.make_async_copy(acc1.at[:, :, pl.ds(lane * 128, 128)], pair_refs[part].at[which, 0, :, slot], sem.at[0, lane]))
                copies.append(pltpu.make_async_copy(acc2.at[:, slot // wide, :, pl.ds(col * 128, 128)], pair_refs[part].at[which, 1, :, slot], sem.at[1, lane]))
            for copy in copies:
                copy.start()
            for copy in copies:
                copy.wait()

    hbm = pl.BlockSpec(memory_space=ANY)
    ops = [first, x, grad, act, slope, w_one, w_two]
    in_specs = [row_spec(d_model), row_spec(d_model), row_spec(d_ff), row_spec(d_ff), weight_spec(d_model, d_ff, which), weight_spec(d_ff, d_model, which)]
    alias = {}
    if pair is not None:
        alias = {len(ops) + part: 1 + part for part in range(n_part)}
        ops += pair
        in_specs += [hbm] * n_part
    out = pl.pallas_call(
        kernel,
        grid_spec=pltpu.PrefetchScalarGridSpec(
            num_scalar_prefetch=1, grid=(n_step,), in_specs=in_specs,
            out_specs=[row_spec(d_model)] + [hbm] * n_part,
            scratch_shapes=[pltpu.VMEM((major, 8, d_ff), F32), pltpu.VMEM((major, per, 8, d_model), F32), pltpu.SemaphoreType.DMA((2, lanes))]),
        out_shape=[jax.ShapeDtypeStruct((n_row, d_model), BF)] + [jax.ShapeDtypeStruct(pair_shape, F32)] * n_part,
        input_output_aliases=alias,
        compiler_params=pltpu.CompilerParams(vmem_limit_bytes=VMEM_CAP, dimension_semantics=("arbitrary",)),
        cost_estimate=pl.CostEstimate(flops=8 * n_row * d_model * d_ff, bytes_accessed=n_row * d_ff * 6, transcendentals=0),
        name="block_bwd",
    )(*ops)
    return out[0], list(out[1:])


def last_call(first, x, grad, act, slope, w_two, which, buf, part, n_part):
    n_row, d_model = grad.shape
    d_ff = w_two.shape[1]
    n_step = n_row // TM
    wide1, wide2 = d_ff // n_part, d_model // n_part
    major = d_model // 8
    per = d_ff // d_model

    def kernel(off_ref, x_ref, g_ref, a_ref, s_ref, w2_ref, old_ref, buf_ref, acc1, acc2, sem):
        step = pl.program_id(0)

        @pl.when(step == 0)
        def _():
            acc1[...] = jnp.zeros_like(acc1)
            acc2[...] = jnp.zeros_like(acc2)

        r = (dot_nt(g_ref[...], w2_ref[...]) * s_ref[...]).astype(BF)
        acc1[...] += dot_tn(x_ref[...], r).reshape(major, 8, wide1)
        acc2[...] += dot_tn(a_ref[...], g_ref[:, part * wide2:(part + 1) * wide2]).reshape(major, per, 8, wide2)

        @pl.when(step == n_step - 1)
        def _():
            copies = []
            for lane in range(wide1 // 128):
                tiles = wide2 // 128
                copies.append(pltpu.make_async_copy(acc1.at[:, :, pl.ds(lane * 128, 128)], buf_ref.at[which, 0, :, lane], sem.at[0, lane]))
                copies.append(pltpu.make_async_copy(acc2.at[:, lane // tiles, :, pl.ds(lane % tiles * 128, 128)], buf_ref.at[which, 1, :, lane], sem.at[1, lane]))
            for copy in copies:
                copy.start()
            for copy in copies:
                copy.wait()

    hbm = pl.BlockSpec(memory_space=ANY)
    part_spec = pl.BlockSpec((TM, wide1), lambda i, off: (i, part))
    w2_spec = pl.BlockSpec((None, wide1, d_model), lambda i, off: (which, part, 0), pipeline_mode=pl.Buffered(1))
    return pl.pallas_call(
        kernel,
        grid_spec=pltpu.PrefetchScalarGridSpec(
            num_scalar_prefetch=1, grid=(n_step,),
            in_specs=[row_spec(d_model, True), row_spec(d_model), row_spec(d_ff), part_spec, w2_spec, hbm],
            out_specs=hbm,
            scratch_shapes=[pltpu.VMEM((major, 8, wide1), F32), pltpu.VMEM((major, per, 8, wide2), F32), pltpu.SemaphoreType.DMA((2, wide1 // 128))]),
        out_shape=jax.ShapeDtypeStruct(buf.shape, F32),
        input_output_aliases={6: 0},
        compiler_params=pltpu.CompilerParams(vmem_limit_bytes=VMEM_CAP, dimension_semantics=("arbitrary",)),
        cost_estimate=pl.CostEstimate(flops=6 * n_row * d_model * wide1, bytes_accessed=n_row * d_ff * 4, transcendentals=0),
        name="block_last",
    )(first, x, grad, act, slope, w_two, buf)


def untile_rows(rows, r, c):
    return rows.reshape(r // 8, c // 128, 8, 128).transpose(0, 2, 1, 3).reshape(r, c)


def adam_call(grads, clip, w_old, m_old, v_old, strides, learn_rate):
    n_row = w_old.shape[0]
    blk = 2304
    n_half = n_row // blk // 2
    n_part = len(grads) - 1
    bc1 = 1.0 / (1.0 - BETA_ONE ** ADAM_STEP)
    bc2 = 1.0 / (1.0 - BETA_TWO ** ADAM_STEP)

    def kernel(c_ref, *refs):
        ga_refs, (gb_ref, w_ref, m_ref, v_ref, wn_ref, mn_ref, vn_ref, wb_ref) = refs[:n_part], refs[n_part:]
        clip_val = c_ref[0, 0]
        data_idx = lax.axis_index("data")

        def run(stride, g_refs):
            n = len(g_refs)
            share = stride // n
            def update(base, lo, tile):
                at = base // n + lo // n + tile % share * 8
                gc = clip_val * g_refs[tile // share][pl.ds(pl.multiple_of(at, 8), 8), :]
                flat = pl.ds(base + lo + tile, 8, stride=stride)
                w = w_ref[flat, :]
                m = BETA_ONE * m_ref[flat, :] + (1.0 - BETA_ONE) * gc
                v = BETA_TWO * v_ref[flat, :] + (1.0 - BETA_TWO) * gc * gc
                mn_ref[flat, :] = m
                vn_ref[flat, :] = v
                new = w - learn_rate * ((m * bc1) / (jnp.sqrt(v * bc2) + ADAM_EPS) + WEIGHT_DECAY * w)
                wn_ref[flat, :] = new
                return new

            def body(i, carry):
                base = pl.multiple_of(i * 192, 192)
                for lo in range(0, 192, 8 * stride):
                    for tile in range(0, stride, 2):
                        pair = jnp.concatenate([update(base, lo, tile), update(base, lo, tile + 1)], axis=0)
                        wb_ref[pl.ds(base + lo + tile * 8, 16), :] = pair.astype(BF)
                return carry

            lax.fori_loop(0, blk // 192, body, 0)

        for half, g_refs in enumerate((ga_refs, (gb_ref,))):
            for kind, stride in enumerate(strides):

                @pl.when((data_idx // 2 == kind) & (pl.program_id(0) // n_half == half))
                def _():
                    run(stride, g_refs)

    spec = pl.BlockSpec((blk, 128), lambda i: (i, 0))
    return pl.pallas_call(
        kernel, grid=(n_row // blk,),
        in_specs=[pl.BlockSpec(memory_space=pltpu.SMEM), *([pl.BlockSpec((blk // n_part, 128), lambda i: (jnp.minimum(i, n_half - 1), 0))] * n_part), pl.BlockSpec((blk, 128), lambda i: (jnp.maximum(i - n_half, 0), 0))] + [spec] * 3,
        out_specs=[spec] * 4,
        out_shape=[jax.ShapeDtypeStruct((n_row, 128), F32)] * 3 + [jax.ShapeDtypeStruct((n_row, 128), BF)],
        compiler_params=pltpu.CompilerParams(vmem_limit_bytes=VMEM_CAP, dimension_semantics=("arbitrary",)),
        name="adam",
    )(clip, *grads, w_old, m_old, v_old)


def solution(mesh):
    n_stage = mesh.shape["stage"]
    n_data = mesh.shape["data"]
    both = ("stage", "data")

    def device_step(x_loc, t_loc, w1_loc, w2_loc, wm_loc, m_loc, v_loc):
        n_micro, n_tok, d_model = x_loc.shape
        d_ff = w1_loc.shape[4]
        n_tokens = n_micro * n_tok * n_data
        n_blocks = 2 * n_stage
        tau_clip = 0.3 * d_model * math.sqrt(n_blocks * (3.0 / n_tokens + 0.008))
        learn_rate = 0.1 / math.sqrt(4.0 * d_model * n_blocks)
        stage_idx = lax.axis_index("stage")
        data_idx = lax.axis_index("data")
        n_mine = n_micro // n_stage
        n_row = n_mine * n_tok
        x_all = x_loc.reshape(n_micro * n_tok, d_model)
        t_all = t_loc.reshape(n_micro * n_tok, d_model)
        first = (stage_idx * (n_row // TM)).astype(jnp.int32).reshape(1)

        def gather(stack, half, after=None):
            part = stack.shape[3] // n_data
            mine = lax.dynamic_slice(stack, (0, half, 0, data_idx * part, 0), (1, 1, 1, part, stack.shape[4])).reshape(part, stack.shape[4])
            if after is not None:
                mine = lax.optimization_barrier((mine, after))[0]
            full = lax.all_gather(mine, both, axis=0, tiled=True)
            return full.reshape(n_stage, *stack.shape[3:])

        ones, twos = [None, None], [None, None]
        ones[0] = gather(w1_loc, 0)
        twos[0] = gather(w2_loc, 0, ones[0])
        ones[1] = gather(w1_loc, 1, twos[0])
        twos[1] = gather(w2_loc, 1, twos[0])

        cur, saved = x_all, []
        for blk in range(n_blocks):
            tail = dict(targets=t_all, n_tokens=n_tokens) if blk == n_blocks - 1 else {}
            if blk == 0:
                act, slope = up_call(first, cur, ones[0], 0, n_row)
                saved.append((cur, act, slope))
                cur = down_call(first, cur, act, twos[0], 0, n_row)
                continue
            outs = fwd_call(first, cur, ones[blk // 2], twos[blk // 2], blk % 2, n_row, **tail)
            saved.append((cur, outs[1], outs[2]))
            cur = outs[0]
        loss_acc = 0.5 * jnp.sum(outs[3])
        grad = cur

        def scatter(buf):
            return lax.psum_scatter(buf.reshape(n_stage * n_data, -1, 128), both, scatter_dimension=0, tiled=True)[0]

        def backward(blk, pair, n_part):
            inp, act, slope = saved[blk]
            return bwd_call(first, inp, grad, act, slope, ones[blk // 2], twos[blk // 2], blk % 2, pair, n_part)

        grad, pair = backward(3, None, 1)
        grad, pair = backward(2, pair, 1)
        late = scatter(pair[0])
        grad, bufs = backward(1, None, N_PART)
        inp, act, slope = saved[0]
        early = []
        for part in range(N_PART):
            early.append(scatter(last_call(first, inp, grad, act, slope, twos[0], 0, bufs[part], part, N_PART)))
        shards = early + [late]
        sq = sum(jnp.sum(s * s) for s in shards)
        sums = lax.psum(jnp.stack([sq, loss_acc]), both)
        clip = jnp.minimum(1.0, tau_clip / jnp.sqrt(sums[0])).reshape(1, 1)
        flat = lambda arr: arr.reshape(-1, 128)
        w_new, m_new, v_new, w_bf = adam_call(shards, clip, flat(wm_loc), flat(m_loc), flat(v_loc), (d_ff // 128, d_model // 128), learn_rate)
        w_full = lax.all_gather(w_bf.reshape(2, 1, -1, 128), "data", axis=1, tiled=True)
        w1_new = untile_rows(w_full[:, :2].reshape(-1, 128), 2 * d_model, d_ff).reshape(w1_loc.shape)
        w2_new = untile_rows(w_full[:, 2:].reshape(-1, 128), 2 * d_ff, d_model).reshape(w2_loc.shape)
        return w1_new, w2_new, w_new.reshape(wm_loc.shape), m_new.reshape(m_loc.shape), v_new.reshape(v_loc.shape), sums[1] / n_tokens

    act_spec = P(None, "data", None)
    flat_spec = P("stage", None, None, "data")
    return jax.shard_map(device_step, mesh=mesh, in_specs=(act_spec, act_spec, P("stage"), P("stage"), flat_spec, flat_spec, flat_spec), out_specs=(P("stage"), P("stage"), flat_spec, flat_spec, flat_spec, P()), check_vma=False)
```

```python
import math
import jax
import jax.numpy as jnp
from jax import lax
from jax.experimental import pallas as pl
from jax.experimental.pallas import tpu as pltpu
from jax.sharding import PartitionSpec as P

BETA_ONE = 0.9
BETA_TWO = 0.999
ADAM_EPS = 1e-8
WEIGHT_DECAY = 0.1
ADAM_STEP = 1000
BF = jnp.bfloat16
F32 = jnp.float32
K_GELU = math.sqrt(2.0 / math.pi)
C_GELU = 0.044715
ANY = pl.ANY
TM = 512
N_PART = 3
VMEM_CAP = 60 * 1024 * 1024


def dot_nn(lhs, rhs):
    return lax.dot_general(lhs, rhs, (((1,), (0,)), ((), ())), preferred_element_type=F32)


def dot_nt(lhs, rhs):
    return lax.dot_general(lhs, rhs, (((1,), (1,)), ((), ())), preferred_element_type=F32)


def dot_tn(lhs, rhs):
    return lax.dot_general(lhs, rhs, (((0,), (0,)), ((), ())), preferred_element_type=F32)


def gelu_and_slope(u):
    sq = u * u
    half = jax.nn.sigmoid(u * (2.0 * K_GELU + (2.0 * K_GELU * C_GELU) * sq))
    act = u * half
    slope = half + (act * (1.0 - half)) * (2.0 * K_GELU + (6.0 * K_GELU * C_GELU) * sq)
    return act, slope


def row_spec(width, moved=False):
    if moved:
        return pl.BlockSpec((TM, width), lambda i, off: (i + off[0], 0))
    return pl.BlockSpec((TM, width), lambda i, off: (i, 0))


def weight_spec(r, c, which):
    return pl.BlockSpec((None, r, c), lambda i, off: (which, 0, 0), pipeline_mode=pl.Buffered(1))


def fwd_call(first, x, w_one, w_two, which, n_row, targets=None, n_tokens=None, chunk=1024):
    d_model = x.shape[1]
    d_ff = w_one.shape[2]
    last = targets is not None

    def kernel(off_ref, x_ref, w1_ref, w2_ref, *rest):
        if last:
            t_ref, h_ref, a_ref, s_ref, loss_ref = rest
        else:
            h_ref, a_ref, s_ref = rest
        acc = x_ref[...].astype(F32)
        pre = dot_nn(x_ref[...], w1_ref[:, :chunk])
        for lo in range(0, d_ff, chunk):
            cols = slice(lo, lo + chunk)
            ahead = dot_nn(x_ref[...], w1_ref[:, lo + chunk:lo + 2 * chunk]) if lo + chunk < d_ff else None
            act, slope = gelu_and_slope(pre)
            act = act.astype(BF)
            a_ref[:, cols] = act
            s_ref[:, cols] = slope
            acc = acc + dot_nn(act, w2_ref[cols, :])
            pre = ahead
        out = acc.astype(BF)
        if not last:
            h_ref[...] = out
        else:
            residual = out.astype(F32) - t_ref[...].astype(F32)
            h_ref[...] = (residual / n_tokens).astype(BF)
            part = jnp.sum((residual * residual).reshape(TM // 8, 8, d_model), axis=0)

            @pl.when(pl.program_id(0) == 0)
            def _():
                loss_ref[...] = part

            @pl.when(pl.program_id(0) > 0)
            def _():
                loss_ref[...] += part

    out_specs = [row_spec(d_model), row_spec(d_ff), row_spec(d_ff)]
    out_shape = [jax.ShapeDtypeStruct((n_row, d_model), BF), jax.ShapeDtypeStruct((n_row, d_ff), BF), jax.ShapeDtypeStruct((n_row, d_ff), F32)]
    if last:
        out_specs.append(pl.BlockSpec((8, d_model), lambda i, off: (0, 0)))
        out_shape.append(jax.ShapeDtypeStruct((8, d_model), F32))
    return pl.pallas_call(
        kernel,
        grid_spec=pltpu.PrefetchScalarGridSpec(
            num_scalar_prefetch=1, grid=(n_row // TM,),
            in_specs=[row_spec(d_model), weight_spec(d_model, d_ff, which), weight_spec(d_ff, d_model, which)] + ([row_spec(d_model, True)] if last else []),
            out_specs=out_specs),
        out_shape=out_shape,
        compiler_params=pltpu.CompilerParams(vmem_limit_bytes=VMEM_CAP, dimension_semantics=("arbitrary",)),
        cost_estimate=pl.CostEstimate(flops=4 * n_row * d_model * d_ff, bytes_accessed=n_row * d_ff * 6, transcendentals=n_row * d_ff),
        name="block_fwd",
    )(first, x, w_one, w_two, *([targets] if last else []))


def up_call(first, x, w_one, which, n_row, chunk=1024):
    d_model = x.shape[1]
    d_ff = w_one.shape[2]

    def kernel(off_ref, x_ref, w1_ref, a_ref, s_ref):
        pre = dot_nn(x_ref[...], w1_ref[:, :chunk])
        for lo in range(0, d_ff, chunk):
            cols = slice(lo, lo + chunk)
            ahead = dot_nn(x_ref[...], w1_ref[:, lo + chunk:lo + 2 * chunk]) if lo + chunk < d_ff else None
            act, slope = gelu_and_slope(pre)
            a_ref[:, cols] = act.astype(BF)
            s_ref[:, cols] = slope
            pre = ahead

    return pl.pallas_call(
        kernel,
        grid_spec=pltpu.PrefetchScalarGridSpec(
            num_scalar_prefetch=1, grid=(n_row // TM,),
            in_specs=[row_spec(d_model, True), weight_spec(d_model, d_ff, which)],
            out_specs=[row_spec(d_ff), row_spec(d_ff)]),
        out_shape=[jax.ShapeDtypeStruct((n_row, d_ff), BF), jax.ShapeDtypeStruct((n_row, d_ff), F32)],
        compiler_params=pltpu.CompilerParams(vmem_limit_bytes=VMEM_CAP, dimension_semantics=("arbitrary",)),
        cost_estimate=pl.CostEstimate(flops=2 * n_row * d_model * d_ff, bytes_accessed=n_row * d_ff * 6, transcendentals=n_row * d_ff),
        name="block_up",
    )(first, x, w_one)


def down_call(first, x, act, w_two, which, n_row):
    d_model = x.shape[1]
    d_ff = w_two.shape[1]

    def kernel(off_ref, x_ref, a_ref, w2_ref, h_ref):
        h_ref[...] = (x_ref[...].astype(F32) + dot_nn(a_ref[...], w2_ref[...])).astype(BF)

    return pl.pallas_call(
        kernel,
        grid_spec=pltpu.PrefetchScalarGridSpec(
            num_scalar_prefetch=1, grid=(n_row // TM,),
            in_specs=[row_spec(d_model, True), row_spec(d_ff), weight_spec(d_ff, d_model, which)],
            out_specs=row_spec(d_model)),
        out_shape=jax.ShapeDtypeStruct((n_row, d_model), BF),
        compiler_params=pltpu.CompilerParams(vmem_limit_bytes=VMEM_CAP, dimension_semantics=("arbitrary",)),
        cost_estimate=pl.CostEstimate(flops=2 * n_row * d_model * d_ff, bytes_accessed=n_row * d_ff * 2, transcendentals=0),
        name="block_down",
    )(first, x, act, w_two)


def bwd_call(first, x, grad, act, slope, w_one, w_two, which, pair, n_part=1, chunk=1024):
    n_row, d_model = grad.shape
    d_ff = w_one.shape[2]
    n_step = n_row // TM
    lanes = d_ff // 128
    major = d_model // 8
    per = d_ff // d_model
    part_lanes = lanes // n_part
    pair_shape = (2, 2, major, part_lanes, 8, 128)

    def kernel(off_ref, x_ref, g_ref, a_ref, s_ref, w1_ref, w2_ref, *rest):
        if pair is not None:
            rest = rest[n_part:]
        gin_ref, pair_refs, (acc1, acc2, sem) = rest[0], rest[1:1 + n_part], rest[1 + n_part:]
        step = pl.program_id(0)

        @pl.when(step == 0)
        def _():
            acc1[...] = jnp.zeros_like(acc1)
            acc2[...] = jnp.zeros_like(acc2)

        back = g_ref[...].astype(F32)
        for lo in range(0, d_ff, chunk):
            cols = slice(lo, lo + chunk)
            r = (dot_nt(g_ref[...], w2_ref[cols, :]) * s_ref[:, cols]).astype(BF)
            acc1[:, :, cols] += dot_tn(x_ref[...], r).reshape(major, 8, chunk)
            n_grp = chunk // (8 * per)
            acc2[lo // (8 * per):lo // (8 * per) + n_grp] += dot_tn(a_ref[:, cols], g_ref[...]).reshape(n_grp, per, 8, d_model)
            back = back + dot_nt(r, w1_ref[:, cols])
        gin_ref[...] = back.astype(BF)

        @pl.when(step == n_step - 1)
        def _():
            copies = []
            for lane in range(lanes):
                part, slot = lane // part_lanes, lane % part_lanes
                wide = part_lanes // per
                col = part * wide + slot % wide
                copies.append(pltpu.make_async_copy(acc1.at[:, :, pl.ds(lane * 128, 128)], pair_refs[part].at[which, 0, :, slot], sem.at[0, lane]))
                copies.append(pltpu.make_async_copy(acc2.at[:, slot // wide, :, pl.ds(col * 128, 128)], pair_refs[part].at[which, 1, :, slot], sem.at[1, lane]))
            for copy in copies:
                copy.start()
            for copy in copies:
                copy.wait()

    hbm = pl.BlockSpec(memory_space=ANY)
    ops = [first, x, grad, act, slope, w_one, w_two]
    in_specs = [row_spec(d_model), row_spec(d_model), row_spec(d_ff), row_spec(d_ff), weight_spec(d_model, d_ff, which), weight_spec(d_ff, d_model, which)]
    alias = {}
    if pair is not None:
        alias = {len(ops) + part: 1 + part for part in range(n_part)}
        ops += pair
        in_specs += [hbm] * n_part
    out = pl.pallas_call(
        kernel,
        grid_spec=pltpu.PrefetchScalarGridSpec(
            num_scalar_prefetch=1, grid=(n_step,), in_specs=in_specs,
            out_specs=[row_spec(d_model)] + [hbm] * n_part,
            scratch_shapes=[pltpu.VMEM((major, 8, d_ff), F32), pltpu.VMEM((major, per, 8, d_model), F32), pltpu.SemaphoreType.DMA((2, lanes))]),
        out_shape=[jax.ShapeDtypeStruct((n_row, d_model), BF)] + [jax.ShapeDtypeStruct(pair_shape, F32)] * n_part,
        input_output_aliases=alias,
        compiler_params=pltpu.CompilerParams(vmem_limit_bytes=VMEM_CAP, dimension_semantics=("arbitrary",)),
        cost_estimate=pl.CostEstimate(flops=8 * n_row * d_model * d_ff, bytes_accessed=n_row * d_ff * 6, transcendentals=0),
        name="block_bwd",
    )(*ops)
    return out[0], list(out[1:])


def last_call(first, x, grad, act, slope, w_two, which, buf, part, n_part):
    n_row, d_model = grad.shape
    d_ff = w_two.shape[1]
    n_step = n_row // TM
    wide1, wide2 = d_ff // n_part, d_model // n_part
    major = d_model // 8
    per = d_ff // d_model

    def kernel(off_ref, x_ref, g_ref, a_ref, s_ref, w2_ref, old_ref, buf_ref, acc1, acc2, sem):
        step = pl.program_id(0)

        @pl.when(step == 0)
        def _():
            acc1[...] = jnp.zeros_like(acc1)
            acc2[...] = jnp.zeros_like(acc2)

        r = (dot_nt(g_ref[...], w2_ref[...]) * s_ref[...]).astype(BF)
        acc1[...] += dot_tn(x_ref[...], r).reshape(major, 8, wide1)
        acc2[...] += dot_tn(a_ref[...], g_ref[:, part * wide2:(part + 1) * wide2]).reshape(major, per, 8, wide2)

        @pl.when(step == n_step - 1)
        def _():
            copies = []
            for lane in range(wide1 // 128):
                tiles = wide2 // 128
                copies.append(pltpu.make_async_copy(acc1.at[:, :, pl.ds(lane * 128, 128)], buf_ref.at[which, 0, :, lane], sem.at[0, lane]))
                copies.append(pltpu.make_async_copy(acc2.at[:, lane // tiles, :, pl.ds(lane % tiles * 128, 128)], buf_ref.at[which, 1, :, lane], sem.at[1, lane]))
            for copy in copies:
                copy.start()
            for copy in copies:
                copy.wait()

    hbm = pl.BlockSpec(memory_space=ANY)
    part_spec = pl.BlockSpec((TM, wide1), lambda i, off: (i, part))
    w2_spec = pl.BlockSpec((None, wide1, d_model), lambda i, off: (which, part, 0), pipeline_mode=pl.Buffered(1))
    return pl.pallas_call(
        kernel,
        grid_spec=pltpu.PrefetchScalarGridSpec(
            num_scalar_prefetch=1, grid=(n_step,),
            in_specs=[row_spec(d_model, True), row_spec(d_model), row_spec(d_ff), part_spec, w2_spec, hbm],
            out_specs=hbm,
            scratch_shapes=[pltpu.VMEM((major, 8, wide1), F32), pltpu.VMEM((major, per, 8, wide2), F32), pltpu.SemaphoreType.DMA((2, wide1 // 128))]),
        out_shape=jax.ShapeDtypeStruct(buf.shape, F32),
        input_output_aliases={6: 0},
        compiler_params=pltpu.CompilerParams(vmem_limit_bytes=VMEM_CAP, dimension_semantics=("arbitrary",)),
        cost_estimate=pl.CostEstimate(flops=6 * n_row * d_model * wide1, bytes_accessed=n_row * d_ff * 4, transcendentals=0),
        name="block_last",
    )(first, x, grad, act, slope, w_two, buf)


def adam_call(grads, clip, w_old, m_old, v_old, half, filled, strides, learn_rate):
    n_row = w_old.shape[0]
    blk = 2304
    n_half = n_row // blk // 2
    n_part = len(grads)
    bc1 = 1.0 / (1.0 - BETA_ONE ** ADAM_STEP)
    bc2 = 1.0 / (1.0 - BETA_TWO ** ADAM_STEP)

    def kernel(c_ref, *refs):
        g_refs, (w_ref, m_ref, v_ref), (wn_ref, mn_ref, vn_ref, wb_ref) = refs[:n_part], refs[n_part:n_part + 3], refs[-4:]
        clip_val = c_ref[0, 0]
        data_idx = lax.axis_index("data")

        def run(stride):
            share = stride // n_part

            def update(base, lo, tile):
                at = base // n_part + lo // n_part + tile % share * 8
                gc = clip_val * g_refs[tile // share][pl.ds(pl.multiple_of(at, 8), 8), :]
                flat = pl.ds(base + lo + tile, 8, stride=stride)
                w = w_ref[flat, :]
                m = BETA_ONE * m_ref[flat, :] + (1.0 - BETA_ONE) * gc
                v = BETA_TWO * v_ref[flat, :] + (1.0 - BETA_TWO) * gc * gc
                mn_ref[flat, :] = m
                vn_ref[flat, :] = v
                new = w - learn_rate * ((m * bc1) / (jnp.sqrt(v * bc2) + ADAM_EPS) + WEIGHT_DECAY * w)
                wn_ref[flat, :] = new
                return new

            def body(i, carry):
                base = pl.multiple_of(i * 192, 192)
                for lo in range(0, 192, 8 * stride):
                    for tile in range(0, stride, 2):
                        pair = jnp.concatenate([update(base, lo, tile), update(base, lo, tile + 1)], axis=0)
                        wb_ref[pl.ds(base + lo + tile * 8, 16), :] = pair.astype(BF)
                return carry

            lax.fori_loop(0, blk // 192, body, 0)

        for kind, stride in enumerate(strides):

            @pl.when(data_idx // 2 == kind)
            def _():
                run(stride)

    spec = pl.BlockSpec((blk, 128), lambda i: (i + half * n_half, 0))
    hbm = pl.BlockSpec(memory_space=ANY)
    return pl.pallas_call(
        kernel, grid=(n_half,),
        in_specs=[pl.BlockSpec(memory_space=pltpu.SMEM)] + [pl.BlockSpec((blk // n_part, 128), lambda i: (i, 0))] * n_part + [spec] * 3 + [hbm] * len(filled),
        out_specs=[spec] * 3 + [pl.BlockSpec((blk, 128), lambda i: (i, 0))],
        out_shape=[jax.ShapeDtypeStruct((n_row, 128), F32)] * 3 + [jax.ShapeDtypeStruct((n_row // 2, 128), BF)],
        input_output_aliases={4 + n_part + k: k for k in range(len(filled))},
        compiler_params=pltpu.CompilerParams(vmem_limit_bytes=VMEM_CAP, dimension_semantics=("arbitrary",)),
        cost_estimate=pl.CostEstimate(flops=20 * n_row * 64, bytes_accessed=n_row * 64 * 30, transcendentals=0),
        name="adam",
    )(clip, *grads, w_old, m_old, v_old, *filled)


def place_call(rows, half, filled, d_model, d_ff):
    n_one = d_model * d_ff // 1024
    lanes1, lanes2 = d_ff // 128, d_model // 128
    steps = 12
    step1, step2 = d_model // 8 // steps, d_ff // 8 // steps

    def kernel(one_ref, two_ref, *refs):
        w1_ref, w2_ref = refs[-2:]
        for lane in range(lanes1):
            w1_ref[:, :, lane * 128:(lane + 1) * 128] = one_ref[:, lane]
        for lane in range(lanes2):
            w2_ref[:, :, lane * 128:(lane + 1) * 128] = two_ref[:, lane]

    hbm = pl.BlockSpec(memory_space=ANY)
    return pl.pallas_call(
        kernel, grid=(steps,),
        in_specs=[pl.BlockSpec((step1, lanes1, 8, 128), lambda i: (i, 0, 0, 0)), pl.BlockSpec((step2, lanes2, 8, 128), lambda i: (steps + i, 0, 0, 0))] + [hbm] * len(filled),
        out_specs=[pl.BlockSpec((None, step1, 8, d_ff), lambda i: (half, i, 0, 0)), pl.BlockSpec((None, step2, 8, d_model), lambda i: (half, i, 0, 0))],
        out_shape=[jax.ShapeDtypeStruct((2, d_model // 8, 8, d_ff), BF), jax.ShapeDtypeStruct((2, d_ff // 8, 8, d_model), BF)],
        input_output_aliases={2 + k: k for k in range(len(filled))},
        compiler_params=pltpu.CompilerParams(vmem_limit_bytes=VMEM_CAP, dimension_semantics=("arbitrary",)),
        cost_estimate=pl.CostEstimate(flops=n_one * 1024, bytes_accessed=n_one * 8192, transcendentals=0),
        name="place",
    )(rows.reshape(-1, lanes1, 8, 128), rows.reshape(-1, lanes2, 8, 128), *filled)


def sum_call(part, n_stage, n_data):
    n_dev = n_stage * n_data

    def kernel(x_ref, o_ref, slots, send_sem, recv_sem):
        me = lax.axis_index("stage") * n_data + lax.axis_index("data")
        barrier = pltpu.get_barrier_semaphore()
        peers = []
        for k in range(1, n_dev):
            other = lax.rem(me + k, n_dev)
            peers.append((lax.div(other, n_data), lax.rem(other, n_data)))
        for peer in peers:
            pl.semaphore_signal(barrier, inc=1, device_id=peer, device_id_type=pl.DeviceIdType.MESH)
        pl.semaphore_wait(barrier, n_dev - 1)
        copies = []
        for k, peer in enumerate(peers, 1):
            copies.append(pltpu.make_async_remote_copy(
                src_ref=x_ref, dst_ref=slots.at[k], send_sem=send_sem.at[k], recv_sem=recv_sem.at[k],
                device_id=peer, device_id_type=pl.DeviceIdType.MESH))
        for copy in copies:
            copy.start()
        slots[0] = x_ref[...]
        for copy in copies:
            copy.wait()
        total = jnp.zeros_like(x_ref)
        for dev in range(n_dev):
            total = total + slots[lax.rem(me - dev + n_dev, n_dev)]
        o_ref[...] = total

    vmem = pl.BlockSpec(memory_space=pltpu.VMEM)
    return pl.pallas_call(
        kernel, in_specs=[vmem], out_specs=vmem,
        out_shape=jax.ShapeDtypeStruct(part.shape, F32),
        scratch_shapes=[pltpu.VMEM((n_dev, *part.shape), F32), pltpu.SemaphoreType.DMA((n_dev,)), pltpu.SemaphoreType.DMA((n_dev,))],
        compiler_params=pltpu.CompilerParams(collective_id=0, has_side_effects=True),
        name="small_sum",
    )(part)


def solution(mesh):
    n_stage = mesh.shape["stage"]
    n_data = mesh.shape["data"]
    both = ("stage", "data")

    def device_step(x_loc, t_loc, w1_loc, w2_loc, wm_loc, m_loc, v_loc):
        n_micro, n_tok, d_model = x_loc.shape
        d_ff = w1_loc.shape[4]
        n_tokens = n_micro * n_tok * n_data
        n_blocks = 2 * n_stage
        tau_clip = 0.3 * d_model * math.sqrt(n_blocks * (3.0 / n_tokens + 0.008))
        learn_rate = 0.1 / math.sqrt(4.0 * d_model * n_blocks)
        stage_idx = lax.axis_index("stage")
        data_idx = lax.axis_index("data")
        n_mine = n_micro // n_stage
        n_row = n_mine * n_tok
        x_all = x_loc.reshape(n_micro * n_tok, d_model)
        t_all = t_loc.reshape(n_micro * n_tok, d_model)
        first = (stage_idx * (n_row // TM)).astype(jnp.int32).reshape(1)

        def gather(stack, half, after=None):
            part = stack.shape[3] // n_data
            mine = lax.dynamic_slice(stack, (0, half, 0, data_idx * part, 0), (1, 1, 1, part, stack.shape[4])).reshape(part, stack.shape[4])
            if after is not None:
                mine = lax.optimization_barrier((mine, after))[0]
            full = lax.all_gather(mine, both, axis=0, tiled=True)
            return full.reshape(n_stage, *stack.shape[3:])

        ones, twos = [None, None], [None, None]
        ones[0] = gather(w1_loc, 0)
        twos[0] = gather(w2_loc, 0, ones[0])
        ones[1] = gather(w1_loc, 1, twos[0])
        twos[1] = gather(w2_loc, 1, twos[0])

        cur, saved = x_all, []
        for blk in range(n_blocks):
            tail = dict(targets=t_all, n_tokens=n_tokens) if blk == n_blocks - 1 else {}
            if blk == 0:
                act, slope = up_call(first, cur, ones[0], 0, n_row)
                saved.append((cur, act, slope))
                cur = down_call(first, cur, act, twos[0], 0, n_row)
                continue
            outs = fwd_call(first, cur, ones[blk // 2], twos[blk // 2], blk % 2, n_row, **tail)
            saved.append((cur, outs[1], outs[2]))
            cur = outs[0]
        loss_rows = jnp.sum(outs[3].reshape(8, -1, 128), axis=1)
        grad = cur

        def scatter(buf):
            return lax.psum_scatter(buf.reshape(n_stage * n_data, -1, 128), both, scatter_dimension=0, tiled=True)[0]

        def backward(blk, pair, n_part):
            inp, act, slope = saved[blk]
            return bwd_call(first, inp, grad, act, slope, ones[blk // 2], twos[blk // 2], blk % 2, pair, n_part)

        grad, pair = backward(3, None, 1)
        grad, pair = backward(2, pair, 1)
        late = scatter(pair[0])
        grad, bufs = backward(1, None, N_PART)
        inp, act, slope = saved[0]
        early = []
        for part in range(N_PART):
            buf = last_call(first, inp, grad, act, slope, twos[0], 0, bufs[part], part, N_PART)
            early.append(scatter(buf))
        fold = lambda arr: jnp.sum(arr.reshape(-1, 8, 128), axis=0)
        squares = sum(fold(shard * shard) for shard in [late] + early)
        sums = sum_call(jnp.concatenate([squares, loss_rows], 0), n_stage, n_data)
        clip = jnp.minimum(1.0, tau_clip / jnp.sqrt(jnp.sum(sums[:8]))).reshape(1, 1)
        mean_loss = 0.5 * jnp.sum(sums[8:]) / n_tokens
        flat = lambda arr: arr.reshape(-1, 128)
        strides = (d_ff // 128, d_model // 128)
        state = [flat(wm_loc), flat(m_loc), flat(v_loc)]
        filled, full = [], [None, None]
        for half, grads in ((1, [late]), (0, early)):
            *filled, w_bf = adam_call(grads, clip, *state, half, filled, strides, learn_rate)
            full[half] = lax.all_gather(w_bf, "data", axis=0, tiled=True)
        w_new, m_new, v_new = filled
        placed = []
        for half in (1, 0):
            placed = place_call(full[half], half, placed, d_model, d_ff)
        w1_new = placed[0].reshape(w1_loc.shape)
        w2_new = placed[1].reshape(w2_loc.shape)
        return w1_new, w2_new, w_new.reshape(wm_loc.shape), m_new.reshape(m_loc.shape), v_new.reshape(v_loc.shape), mean_loss

    act_spec = P(None, "data", None)
    flat_spec = P("stage", None, None, "data")
    return jax.shard_map(device_step, mesh=mesh, in_specs=(act_spec, act_spec, P("stage"), P("stage"), flat_spec, flat_spec, flat_spec), out_specs=(P("stage"), P("stage"), flat_spec, flat_spec, flat_spec, P()), check_vma=False)
```
